32 devices in a mesh: ga: 2 (over y), gx: 4 (over z), gy: 2 (over x), col: 2 (over core).
Axes of the slice: x: 2, y: 2, z: 4, core: 2. Of those that a mesh axis runs over, the one named last changes fastest.
Arguments:
- pair_rep: bfloat16 [2, 160, 160, 128], P('ga', 'gx', 'gy'), parts along dimension 0, may hold values from -6 to 6
- pair_mask: int32 [2, 160, 160], P('ga', 'gx', 'gy'), parts along dimension 0, may hold values 0 or 1
- amax_history: float32 [2, 128], P(None, 'col'), may hold values from 0.3 to 3
- in_gain: float32 [128], replicated, may hold values from 0.5 to 1.5
- in_bias: float32 [128], replicated, may hold values from -3 to 3
- proj_weight: bfloat16 [128, 4, 128], P(None, None, 'col'), may hold values from -0.5 to 0.5
- gate_weight: bfloat16 [128, 128], P(None, 'col'), may hold values from -0.5 to 0.5
- out_gain: float32 [128], replicated, may hold values from 0.5 to 1.5
- out_bias: float32 [128], replicated, may hold values from -3 to 3
- out_weight: bfloat16 [128, 128], P(None, 'col'), may hold values from -0.5 to 0.5
Outputs:
- update: bfloat16 [2, 160, 160, 128], P('ga', 'gx', 'gy', 'col'), parts along dimension 0
- new_amax: float32 [4, 128], P('ga', 'col'), parts along dimension 0
The draws below stay inside these ranges and needn't reach their ends.
There are 2 independent parts, one for each index of `ga`. The reference program is written for one: setup_inputs(seed, part) draws one part's arguments, and reference() takes and returns one part's arrays. A program takes and returns all parts, laid end to end along the dimension named above; an argument that names none is the same for every part. Nothing has to cross between parts.
All inputs are finite; a program needn't handle non-finite values. No bound on the sum of `pair_mask` on one device may be relied on, other than what follows from the above.
Results may differ from the reference program's by a relative error of at most 0.0065.
Values may be sent and summed in bfloat16 or wider, within the bound.
A program may use at most 128 MiB of HBM per device.

```python
import math
import jax
import jax.numpy as jnp
from jax import lax

C = 128
CROPS = 1
N = 160


def place_ends(result, stream_key, low, top_value):
    longest = result.shape.index(max(result.shape))
    spots = []
    for shift in (0, 1):
        where = [jax.random.randint(jax.random.fold_in(stream_key, axis), (), 0, length) for axis, length in enumerate(result.shape)]
        where[longest] = (where[longest] + shift) % result.shape[longest]
        spots.append(tuple(where))
    return result.at[spots[0]].set(low).at[spots[1]].set(top_value)


def levels(key, shape, cuts, low, largest):
    level, own = 1.0, jax.random.fold_in(key, 6)
    for axis_at, blocks in cuts:
        heights = jnp.exp(jax.random.uniform(jax.random.fold_in(own, axis_at), (blocks,), jnp.float32, low / len(cuts), largest / len(cuts)))
        level = level * jnp.repeat(heights, shape[axis_at] // blocks).reshape([-1 if axis == axis_at else 1 for axis in range(len(shape))])
    return level


def scatter_about(own_key, extent, scale, reach, pieces=(), held_as=jnp.bfloat16):
    result = scale * jax.random.normal(own_key, extent, jnp.float32)
    if pieces:
        result = result * levels(own_key, extent, pieces, -0.22, 0.18)
    return jnp.clip(result, -reach, reach).astype(held_as)


def setup_inputs(seed: int = 0, part: int = 0) -> dict:
    seeds = jax.random.split(jax.random.key(seed), 11)
    part_keys = jax.random.split(jax.random.fold_in(seeds[10], part), 11)
    pair_rep = scatter_about(part_keys[0], (CROPS, N, N, C), 1.0, 6.0, ((1, 4), (2, 2)))
    pair_mask = place_ends((jax.random.randint(part_keys[1], (CROPS, N, N), 0, 10) < 9).astype(jnp.int32), jax.random.fold_in(part_keys[1], 1), 0, 1)
    amax_history = jnp.clip(jnp.exp(math.log(3.0) - 2.3025851 * jax.random.uniform(seeds[2], (2, C), jnp.float32) ** levels(seeds[2], (2, C), ((1, 2),), -0.2, 0.2)), 0.3, 3.0)
    in_gain = jnp.clip(1.0 + 0.1 * jax.random.normal(seeds[3], (C,), jnp.float32), 0.5, 1.5)
    in_bias = scatter_about(seeds[4], (C,), 0.5, 3.0, (), jnp.float32)
    proj_weight = scatter_about(seeds[5], (C, 4, C), C ** -0.5, 0.5, ((2, 2),))
    gate_weight = scatter_about(seeds[6], (C, C), C ** -0.5, 0.5, ((1, 2),))
    out_gain = jnp.clip(1.0 + 0.1 * jax.random.normal(seeds[7], (C,), jnp.float32), 0.5, 1.5)
    out_bias = scatter_about(seeds[8], (C,), 0.5, 3.0, (), jnp.float32)
    out_weight = scatter_about(seeds[9], (C, C), C ** -0.5, 0.5, ((1, 2),))
    return {"pair_rep": pair_rep, "pair_mask": pair_mask, "amax_history": amax_history, "in_gain": in_gain, "in_bias": in_bias, "proj_weight": proj_weight, "gate_weight": gate_weight, "out_gain": out_gain, "out_bias": out_bias, "out_weight": out_weight}


epsilon = 1e-05
format_limit = 448.0

def layer_norm(values, gain, bias):
    average = lax.optimization_barrier(jnp.mean(values, axis=-1, keepdims=True))
    spread = lax.optimization_barrier(jnp.mean(jnp.square(values - average), axis=-1, keepdims=True))
    return (values - average) * lax.rsqrt(spread + epsilon) * gain + bias

def one_crop(crop_rep, crop_mask, amax_history, in_gain, in_bias, proj_weight, gate_weight, out_gain, out_bias, out_weight):
    normed = layer_norm(crop_rep.astype(jnp.float32), in_gain, in_bias).astype(jnp.bfloat16)
    flat = normed.reshape(N * N, C)
    masking = crop_mask.astype(jnp.float32).reshape(N * N, 1)

    def project(which):
        return jnp.dot(flat, proj_weight[:, which, :], preferred_element_type=jnp.float32)
    left_proj = masking * jax.nn.sigmoid(project(1)) * project(0)
    right_proj = masking * jax.nn.sigmoid(project(3)) * project(2)
    crop_amax = jnp.stack([lax.optimization_barrier(jnp.max(jnp.abs(left_proj), axis=0)), lax.optimization_barrier(jnp.max(jnp.abs(right_proj), axis=0))])
    scales = amax_history / format_limit
    left_q = jnp.clip(left_proj / scales[0], -format_limit, format_limit).astype(jnp.bfloat16).reshape(N, N, C)
    right_q = jnp.clip(right_proj / scales[1], -format_limit, format_limit).astype(jnp.bfloat16).reshape(N, N, C)
    products = jnp.einsum('ikc,jkc->ijc', left_q.astype(jnp.float32), right_q.astype(jnp.float32))
    triangle = (products * (scales[0] * scales[1])).astype(jnp.bfloat16)
    tnorm = layer_norm(triangle.astype(jnp.float32), out_gain, out_bias).astype(jnp.bfloat16)
    gating = jax.nn.sigmoid(jnp.dot(flat, gate_weight, preferred_element_type=jnp.float32))
    mixing = jnp.dot(tnorm.reshape(N * N, C), out_weight, preferred_element_type=jnp.float32)
    update = (gating * mixing).astype(jnp.bfloat16).reshape(N, N, C)
    return (update, crop_amax)

def reference(pair_rep, pair_mask, amax_history, in_gain, in_bias, proj_weight, gate_weight, out_gain, out_bias, out_weight):
    updates = []
    maxima = []
    for crop in range(CROPS):
        update, crop_amax = one_crop(pair_rep[crop], pair_mask[crop], amax_history, in_gain, in_bias, proj_weight, gate_weight, out_gain, out_bias, out_weight)
        updates.append(update)
        maxima.append(crop_amax)
    new_amax = maxima[0]
    for crop_amax in maxima[1:]:
        new_amax = jnp.maximum(new_amax, crop_amax)
    return (jnp.stack(updates), new_amax)
```

```python
import functools

import jax
import jax.numpy as jnp
from jax import lax
from jax.experimental import pallas as pl
from jax.experimental.pallas import tpu as pltpu
from jax.sharding import PartitionSpec as P

epsilon = 1e-05
format_limit = 448.0
LANES = 128
f32, bf16 = jnp.float32, jnp.bfloat16
MESH = pl.DeviceIdType.MESH


def kernel(
    dims,
    rep_ref,
    mask_ref,
    hist_ref,
    hist_smem,
    in_gain_ref,
    in_bias_ref,
    proj_ref,
    gate_ref,
    out_gain_smem,
    out_bias_smem,
    out_weight_ref,
    out_ref,
    amax_ref,
    normed,
    maskf,
    inverse,
    peak,
    left_s,
    right_s,
    left_b,
    right_all,
    own_t,
    send_t,
    recv_t,
    full_t,
    spread_t,
    mix_w,
    ow_pad,
    gating,
    peaks,
    peak_send,
    peak_recv,
    z_send,
    z_recv,
    x_send,
    x_recv,
    c_send,
    c_recv,
):
    nz, ny, rows, cols, half, chunks = dims
    ratio = nz // ny
    channels = 2 * half
    per = LANES // rows
    pairs = -(-half // (2 * per))
    groups = 2 * pairs
    span = per * rows
    slot = LANES // (2 * ratio)
    z, y, col = lax.axis_index("gx"), lax.axis_index("gy"), lax.axis_index("col")
    members = nz * ny
    me = z * ny + y

    barrier = pltpu.get_barrier_semaphore()

    def greet(t, carry):
        peer = lax.rem(me + t, members)
        pl.semaphore_signal(
            barrier, inc=1, device_id={"gx": peer // ny, "gy": lax.rem(peer, ny)}, device_id_type=MESH
        )
        return carry

    lax.fori_loop(1, members, greet, 0)
    pl.semaphore_signal(barrier, inc=1, device_id={"col": 1 - col}, device_id_type=MESH)

    normed[pl.ds(rows * cols, LANES), :] = jnp.zeros((LANES, channels), bf16)
    step_rows = 4

    def norm_step(b, carry):
        values = rep_ref[pl.ds(b * step_rows, step_rows)].reshape(step_rows * cols, channels).astype(f32)
        average = jnp.mean(values, axis=-1, keepdims=True)
        centred = values - average
        var = jnp.mean(jnp.square(centred), axis=-1, keepdims=True)
        result = centred * lax.rsqrt(var + epsilon) * in_gain_ref[...] + in_bias_ref[...]
        start = pl.multiple_of(b * step_rows * cols, 16)
        normed[pl.ds(start, step_rows * cols), :] = result.astype(bf16)
        return carry

    lax.fori_loop(0, rows // step_rows, norm_step, 0)
    maskf[...] = jnp.zeros_like(maskf)
    maskf[:, 0:cols] = mask_ref[...].astype(f32)
    flipped = jnp.broadcast_to(format_limit / hist_ref[...], (channels, channels))
    inverse[...] = jnp.transpose(flipped)
    peak[...] = jnp.zeros_like(peak)
    tail = left_s.shape[0] - half * rows
    left_s[pl.ds(half * rows, tail), :] = jnp.zeros((tail, LANES), f32)
    right_s[pl.ds(half * rows, tail), :] = jnp.zeros((tail, LANES), f32)

    def project(side, target):
        base = side * half

        def one(i):
            block = normed[pl.ds(pl.multiple_of(i * cols, 16), LANES), :]
            p = lax.dot_general(
                proj_ref[2 * base : 2 * base + channels, :],
                block,
                (((1,), (1,)), ((), ())),
                preferred_element_type=f32,
            )
            value = jax.nn.sigmoid(p[half:]) * p[:half] * maskf[pl.ds(i, 1), :]
            target[pl.ds(i, half, stride=rows), :] = jnp.clip(
                value * inverse[base : base + half, :], -format_limit, format_limit
            )
            return jnp.abs(value)

        def step(b, top):
            for u in range(4):
                top = jnp.maximum(top, one(b * 4 + u))
            return top

        top = lax.fori_loop(0, rows // 4, step, jnp.zeros((half, LANES), f32))
        peak[base : base + half, :] = top

    project(1, right_s)
    bounds = [pairs * c // chunks for c in range(chunks + 1)]

    def z_copy(source, c, direction):
        window = pl.ds(2 * bounds[c], 2 * (bounds[c + 1] - bounds[c]))
        toward = z + 1 if direction == 0 else z - 1
        return pltpu.make_async_remote_copy(
            src_ref=right_all.at[source, window],
            dst_ref=right_all.at[source, window],
            send_sem=z_send.at[direction, source, c],
            recv_sem=z_recv.at[source, c],
            device_id={"gx": toward},
            device_id_type=MESH,
        )

    pl.semaphore_wait(barrier, members)
    for c in range(chunks):
        for g in range(2 * bounds[c], 2 * bounds[c + 1]):
            tile = jnp.transpose(right_s[g * span : g * span + LANES, :])
            right_all[z, g] = tile[:cols].astype(bf16)

        @pl.when(z < nz - 1)
        def _():
            z_copy(z, c, 0).start()

        @pl.when(z > 0)
        def _():
            z_copy(z, c, 1).start()

    project(0, left_s)
    for g in range(groups):
        left_b[g] = left_s[g * span : g * span + LANES, :].astype(bf16)

    peaks[me] = jnp.broadcast_to(jnp.max(jnp.transpose(peak[...]), axis=0, keepdims=True), (8, channels))

    def spread_peak(t, carry):
        peer = lax.rem(me + t, members)
        pltpu.make_async_remote_copy(
            src_ref=peaks.at[me],
            dst_ref=peaks.at[me],
            send_sem=peak_send,
            recv_sem=peak_recv,
            device_id={"gx": peer // ny, "gy": lax.rem(peer, ny)},
            device_id_type=MESH,
        ).start()
        return carry

    lax.fori_loop(1, members, spread_peak, 0)

    lane = lax.broadcasted_iota(jnp.int32, (rows, LANES), 1)

    def triangle_pair(r, p):
        halves = []
        for u in range(2):
            res = lax.dot_general(
                left_b[2 * p + u][:, :cols],
                right_all[r, 2 * p + u],
                (((1,), (0,)), ((), ())),
                preferred_element_type=f32,
            )
            t = res[:rows]
            for s in range(1, per):
                t = jnp.where(lane >= s * rows, res[s * rows : (s + 1) * rows], t)
            halves.append(t)
        return jnp.concatenate(halves, axis=0)

    def x_copy(target, sub, c, source):
        window = pl.ds(bounds[c], bounds[c + 1] - bounds[c])
        return pltpu.make_async_remote_copy(
            src_ref=send_t.at[target, sub, window],
            dst_ref=recv_t.at[source, sub, window],
            send_sem=x_send.at[target, sub, c],
            recv_sem=x_recv.at[source, sub, c],
            device_id={"gy": target},
            device_id_type=MESH,
        )

    def triangle_block(r, c):
        owner, sub = r // ratio, lax.rem(r, ratio)

        @pl.when(owner == y)
        def _():
            for p in range(bounds[c], bounds[c + 1]):
                own_t[sub, p] = triangle_pair(r, p)

        @pl.when(owner != y)
        def _():
            for p in range(bounds[c], bounds[c + 1]):
                send_t[owner, sub, p] = triangle_pair(r, p).astype(bf16)
            x_copy(owner, sub, c, y).start()

    def own_block(c):
        triangle_block(z, c)

    for c in range(chunks):
        own_block(c)

    def gate_step(b, carry):
        size = step_rows * cols
        start = pl.multiple_of(b * size, 16)
        gating[pl.ds(start, size), :] = jax.nn.sigmoid(
            jnp.dot(normed[pl.ds(start, size), :], gate_ref[...], preferred_element_type=f32)
        )
        return carry

    lax.fori_loop(0, rows // step_rows, gate_step, 0)
    ow_pad[...] = jnp.zeros_like(ow_pad)
    stretch = ow_pad.shape[0] // 2
    for cc in range(2):
        ow_pad[cc * stretch : cc * stretch + half, 0:half] = out_weight_ref[
            cc * half : (cc + 1) * half, :
        ].astype(f32)
    mix_w[...] = jnp.zeros_like(mix_w)
    for rr in range(ratio):
        for s in range(per):
            for cc in range(2):
                piece = ow_pad[pl.ds(cc * stretch + s, slot, stride=per), :]
                at = rr * 2 * slot + cc * slot
                mix_w[rr, s, at : at + slot, :] = piece.astype(bf16)
    spread_t[...] = jnp.zeros_like(spread_t)

    def ring_step(d, carry):
        low, high = z - d, z + d
        for c in range(chunks):

            @pl.when(low >= 0)
            def _():
                z_copy(low, c, 0).wait_recv()

                @pl.when(z < nz - 1)
                def _():
                    z_copy(low, c, 0).start()

            @pl.when(high < nz)
            def _():
                z_copy(high, c, 1).wait_recv()

                @pl.when(z > 0)
                def _():
                    z_copy(high, c, 1).start()

            @pl.when(low >= 0)
            def _():
                triangle_block(low, c)

            @pl.when(high < nz)
            def _():
                triangle_block(high, c)

        return carry

    lax.fori_loop(1, nz, ring_step, 0)

    group_lane = lax.broadcasted_iota(jnp.int32, (1, LANES), 1)

    def lane_vector(scalar_of):
        vector = jnp.full((1, LANES), scalar_of(0), f32)
        for s in range(1, per):
            vector = jnp.where(group_lane >= s * rows, scalar_of(s), vector)
        return vector

    def pair_vector(scalar_of, p):
        parts = []
        for u in range(2):
            g = 2 * p + u
            vector = lane_vector(lambda s: scalar_of(g * per + s))
            parts.append(jnp.broadcast_to(vector, (rows, LANES)))
        return jnp.concatenate(parts, axis=0)

    def scale_of(ch):
        ch = jnp.minimum(ch, half - 1)
        return (hist_smem[0, ch] / format_limit) * (hist_smem[1, ch] / format_limit)

    def c_copy(sub, c):
        window = pl.ds(bounds[c], bounds[c + 1] - bounds[c])
        return pltpu.make_async_remote_copy(
            src_ref=full_t.at[col, sub, window],
            dst_ref=full_t.at[col, sub, window],
            send_sem=c_send.at[sub, c],
            recv_sem=c_recv.at[sub, c],
            device_id={"col": 1 - col},
            device_id_type=MESH,
        )

    for sub in range(ratio):
        for c in range(chunks):

            def arrive(t, carry):
                x_copy(y, sub, c, lax.rem(y + t, ny)).wait_recv()
                return carry

            lax.fori_loop(1, ny, arrive, 0)

            def finish(p, carry):
                total = own_t[sub, p]
                for t in range(1, ny):
                    total = total + recv_t[lax.rem(y + t, ny), sub, p].astype(f32)
                full_t[col, sub, p] = (total * pair_vector(scale_of, p)).astype(bf16)
                return carry

            lax.fori_loop(bounds[c], bounds[c + 1], finish, 0)
            c_copy(sub, c).start()

    valid = lax.broadcasted_iota(jnp.int32, (2 * rows, LANES), 1) < 0
    row_at = lax.broadcasted_iota(jnp.int32, (2 * rows, LANES), 0) // rows
    lane_at = lax.broadcasted_iota(jnp.int32, (2 * rows, LANES), 1) // rows
    valid = (((pairs - 1) * 2 + row_at) * per + lane_at) < half

    def segment_mean(pair_sum):
        x = pair_sum[:rows] + pair_sum[rows:]
        total = x
        for s in range(1, per):
            total = total + pltpu.roll(x, s * rows, 1)
        result = total
        for s in range(1, per):
            moved = pltpu.roll(total, LANES - s * rows, 1)
            result = jnp.where(lane < (per - s) * rows, moved, result)
        result = result * (1.0 / channels)
        return jnp.concatenate([result, result], axis=0)

    for sub in range(ratio):
        for c in range(chunks):
            c_copy(sub, c).wait_recv()

        def add_up(p, total):
            return total + full_t[0, sub, p].astype(f32) + full_t[1, sub, p].astype(f32)

        zero = jnp.zeros((2 * rows, LANES), f32)
        mean = segment_mean(lax.fori_loop(0, pairs, add_up, zero))

        def add_squares(p, total):
            for cc in range(2):
                total = total + jnp.square(full_t[cc, sub, p].astype(f32) - mean)
            return total

        squares = lax.fori_loop(0, pairs - 1, add_squares, zero)
        for cc in range(2):
            last = jnp.square(full_t[cc, sub, pairs - 1].astype(f32) - mean)
            squares = squares + jnp.where(valid, last, 0.0)
        factor = lax.rsqrt(segment_mean(squares) + epsilon)

        def normalise(p, carry):
            for cc in range(2):

                def gain_of(ch, cc=cc):
                    return out_gain_smem[cc * half + jnp.minimum(ch, half - 1)]

                def bias_of(ch, cc=cc):
                    return out_bias_smem[cc * half + jnp.minimum(ch, half - 1)]

                t = (full_t[cc, sub, p].astype(f32) - mean) * factor
                t = t * pair_vector(gain_of, p) + pair_vector(bias_of, p)
                for u in range(2):
                    at = (sub * 2 + cc) * slot + 2 * p + u
                    spread_t[pl.ds(at, rows, stride=LANES), :] = t[u * rows : (u + 1) * rows]
            return carry

        lax.fori_loop(0, pairs, normalise, 0)

    batch = 8

    def mix_step(b, carry):
        pieces = [[] for _ in range(per)]
        for u in range(batch):
            start = pl.multiple_of((b * batch + u) * LANES, LANES)
            tile = jnp.transpose(spread_t[pl.ds(start, LANES), :])
            for s in range(per):
                pieces[s].append(tile[s * rows : (s + 1) * rows])
        blocks = [jnp.concatenate(piece, axis=0).astype(bf16) for piece in pieces]
        mixed = []
        for rr in range(ratio):
            total = jnp.dot(blocks[0], mix_w[rr, 0], preferred_element_type=f32)
            for s in range(1, per):
                total = total + jnp.dot(blocks[s], mix_w[rr, s], preferred_element_type=f32)
            mixed.append(total[:, :half].reshape(batch, rows, half))
        mixing = jnp.concatenate(mixed, axis=1)
        start = pl.multiple_of(b * batch * cols, 16)
        gates = gating[pl.ds(start, batch * cols), :].reshape(batch, cols, half)
        out_ref[pl.ds(b * batch, batch)] = (gates * mixing).astype(bf16)
        return carry

    lax.fori_loop(0, rows // batch, mix_step, 0)

    others = peaks.at[pl.ds(0, members - 1)]
    pltpu.make_async_copy(others, others, peak_recv).wait()
    top = jnp.max(jnp.max(peaks[...], axis=0), axis=0, keepdims=True)
    amax_ref[0:1, :] = top[:, :half]
    amax_ref[1:2, :] = top[:, half:]

    pltpu.make_async_copy(others, others, peak_send).wait()
    for sub in range(ratio):
        for c in range(chunks):
            c_copy(sub, c).wait_send()

    def drain_x(t, carry):
        for sub in range(ratio):
            for c in range(chunks):
                x_copy(lax.rem(y + t, ny), sub, c, y).wait_send()
        return carry

    lax.fori_loop(1, ny, drain_x, 0)

    def drain_z(source, carry):
        for c in range(chunks):

            @pl.when((source <= z) & (z < nz - 1))
            def _():
                z_copy(source, c, 0).wait_send()

            @pl.when((source >= z) & (z > 0))
            def _():
                z_copy(source, c, 1).wait_send()

        return carry

    lax.fori_loop(0, nz, drain_z, 0)


def on_device(
    nz,
    ny,
    pair_rep,
    pair_mask,
    amax_history,
    in_gain,
    in_bias,
    proj_weight,
    gate_weight,
    out_gain,
    out_bias,
    out_weight,
):
    crops, rows, cols, channels = pair_rep.shape
    half = proj_weight.shape[2]
    chunks = 2
    ratio = nz // ny
    per = LANES // rows
    pairs = -(-half // (2 * per))
    groups = 2 * pairs
    slot = LANES // (2 * ratio)
    members = nz * ny
    weights = jnp.transpose(proj_weight, (1, 2, 0)).reshape(4 * half, channels)
    scratch_rows = -(-((groups - 1) * per * rows + LANES) // 8) * 8
    dma = pltpu.SemaphoreType.DMA
    vmem = pl.BlockSpec(memory_space=pltpu.VMEM)
    smem = pl.BlockSpec(memory_space=pltpu.SMEM)
    tile = (2 * rows, LANES)
    update, new_amax = pl.pallas_call(
        functools.partial(kernel, (nz, ny, rows, cols, half, chunks)),
        out_shape=(
            jax.ShapeDtypeStruct((rows, cols, half), bf16),
            jax.ShapeDtypeStruct((2, half), f32),
        ),
        in_specs=[vmem, vmem, vmem, smem, vmem, vmem, vmem, vmem, smem, smem, vmem],
        out_specs=(vmem, vmem),
        scratch_shapes=[
            pltpu.VMEM((rows * cols + LANES, channels), bf16),
            pltpu.VMEM((rows, LANES), f32),
            pltpu.VMEM((channels, LANES), f32),
            pltpu.VMEM((channels, LANES), f32),
            pltpu.VMEM((scratch_rows, LANES), f32),
            pltpu.VMEM((scratch_rows, LANES), f32),
            pltpu.VMEM((groups, LANES, LANES), bf16),
            pltpu.VMEM((nz, groups, cols, LANES), bf16),
            pltpu.VMEM((ratio, pairs) + tile, f32),
            pltpu.VMEM((ny, ratio, pairs) + tile, bf16),
            pltpu.VMEM((ny, ratio, pairs) + tile, bf16),
            pltpu.VMEM((2, ratio, pairs) + tile, bf16),
            pltpu.VMEM((rows * LANES, LANES), f32),
            pltpu.VMEM((ratio, per, LANES, LANES), bf16),
            pltpu.VMEM((2 * slot * per, LANES), f32),
            pltpu.VMEM((rows * cols, half), f32),
            pltpu.VMEM((members, 8, channels), f32),
            dma,
            dma,
            dma((2, nz, chunks)),
            dma((nz, chunks)),
            dma((ny, ratio, chunks)),
            dma((ny, ratio, chunks)),
            dma((ratio, chunks)),
            dma((ratio, chunks)),
        ],
        compiler_params=pltpu.CompilerParams(
            collective_id=0, has_side_effects=True, vmem_limit_bytes=56 * 1024 * 1024
        ),
    )(
        pair_rep[0],
        pair_mask[0],
        amax_history.reshape(1, channels),
        amax_history,
        in_gain.reshape(1, channels),
        in_bias.reshape(1, channels),
        weights,
        gate_weight,
        out_gain,
        out_bias,
        out_weight,
    )
    return update[None], new_amax


def solution(mesh):
    placed = (
        P("ga", "gx", "gy", None),
        P("ga", "gx", "gy"),
        P(None, "col"),
        P(),
        P(),
        P(None, None, "col"),
        P(None, "col"),
        P(),
        P(),
        P(None, "col"),
    )
    return jax.shard_map(
        functools.partial(on_device, mesh.shape["gx"], mesh.shape["gy"]),
        mesh=mesh,
        in_specs=placed,
        out_specs=(P("ga", "gx", "gy", "col"), P("ga", "col")),
        check_vma=False,
    )
```

```python
import functools

import jax
import jax.numpy as jnp
from jax import lax
from jax.experimental import pallas as pl
from jax.experimental.pallas import tpu as pltpu
from jax.sharding import PartitionSpec as P

epsilon = 1e-05
format_limit = 448.0
LANES = 128
f32, bf16 = jnp.float32, jnp.bfloat16
MESH = pl.DeviceIdType.MESH


def kernel(
    dims,
    rep_ref,
    mask_ref,
    hist_ref,
    hist_smem,
    in_gain_ref,
    in_bias_ref,
    proj_ref,
    gate_ref,
    out_gain_smem,
    out_bias_smem,
    out_weight_ref,
    out_ref,
    amax_ref,
    normed,
    maskf,
    inverse,
    peak,
    left_s,
    right_s,
    left_b,
    right_all,
    own_t,
    send_t,
    recv_t,
    full_t,
    spread_t,
    mix_w,
    ow_pad,
    gating,
    peaks,
    peak_send,
    peak_recv,
    z_send,
    z_recv,
    x_send,
    x_recv,
    c_send,
    c_recv,
):
    nz, ny, rows, cols, half, chunks = dims
    ratio = nz // ny
    channels = 2 * half
    per = LANES // rows
    pairs = -(-half // (2 * per))
    groups = 2 * pairs
    span = per * rows
    slot = LANES // (2 * ratio)
    z, y, col = lax.axis_index("gx"), lax.axis_index("gy"), lax.axis_index("col")
    members = nz * ny
    me = z * ny + y

    barrier = pltpu.get_barrier_semaphore()

    def greet(t, carry):
        peer = lax.rem(me + t, members)
        pl.semaphore_signal(
            barrier, inc=1, device_id={"gx": peer // ny, "gy": lax.rem(peer, ny)}, device_id_type=MESH
        )
        return carry

    lax.fori_loop(1, members, greet, 0)
    pl.semaphore_signal(barrier, inc=1, device_id={"col": 1 - col}, device_id_type=MESH)

    normed[pl.ds(rows * cols, LANES), :] = jnp.zeros((LANES, channels), bf16)
    step_rows = 4

    def norm_step(b, carry):
        values = rep_ref[pl.ds(b * step_rows, step_rows)].reshape(step_rows * cols, channels).astype(f32)
        average = jnp.mean(values, axis=-1, keepdims=True)
        centred = values - average
        var = jnp.mean(jnp.square(centred), axis=-1, keepdims=True)
        result = centred * lax.rsqrt(var + epsilon) * in_gain_ref[...] + in_bias_ref[...]
        start = pl.multiple_of(b * step_rows * cols, 16)
        normed[pl.ds(start, step_rows * cols), :] = result.astype(bf16)
        return carry

    lax.fori_loop(0, rows // step_rows, norm_step, 0)
    maskf[...] = jnp.zeros_like(maskf)
    maskf[:, 0:cols] = mask_ref[...].astype(f32)
    scaled = format_limit / hist_ref[...]
    flipped = jnp.concatenate([scaled[0:1], scaled[1:2]], axis=1)
    flipped = jnp.broadcast_to(flipped, (channels, channels))
    inverse[...] = jnp.transpose(flipped)
    peak[...] = jnp.zeros_like(peak)
    tail = left_s.shape[0] - half * rows
    left_s[pl.ds(half * rows, tail), :] = jnp.zeros((tail, LANES), f32)
    right_s[pl.ds(half * rows, tail), :] = jnp.zeros((tail, LANES), f32)

    def project(side, target):
        base = side * half

        def one(i):
            block = normed[pl.ds(pl.multiple_of(i * cols, 16), LANES), :]
            p = lax.dot_general(
                proj_ref[2 * base : 2 * base + channels, :],
                block,
                (((1,), (1,)), ((), ())),
                preferred_element_type=f32,
            )
            value = jax.nn.sigmoid(p[half:]) * p[:half] * maskf[pl.ds(i, 1), :]
            target[pl.ds(i, half, stride=rows), :] = jnp.clip(
                value * inverse[base : base + half, :], -format_limit, format_limit
            )
            return jnp.abs(value)

        def step(b, top):
            for u in range(4):
                top = jnp.maximum(top, one(b * 4 + u))
            return top

        top = lax.fori_loop(0, rows // 4, step, jnp.zeros((half, LANES), f32))
        peak[base : base + half, :] = top

    project(1, right_s)
    bounds = [pairs * c // chunks for c in range(chunks + 1)]

    def z_copy(source, c, direction):
        window = pl.ds(2 * bounds[c], 2 * (bounds[c + 1] - bounds[c]))
        toward = z + 1 if direction == 0 else z - 1
        return pltpu.make_async_remote_copy(
            src_ref=right_all.at[source, window],
            dst_ref=right_all.at[source, window],
            send_sem=z_send.at[direction, source, c],
            recv_sem=z_recv.at[source, c],
            device_id={"gx": toward},
            device_id_type=MESH,
        )

    pl.semaphore_wait(barrier, members)
    for c in range(chunks):
        for g in range(2 * bounds[c], 2 * bounds[c + 1]):
            tile = jnp.transpose(right_s[g * span : g * span + LANES, :])
            right_all[z, g] = tile[:cols].astype(bf16)

        @pl.when(z < nz - 1)
        def _():
            z_copy(z, c, 0).start()

        @pl.when(z > 0)
        def _():
            z_copy(z, c, 1).start()

    project(0, left_s)
    for g in range(groups):
        left_b[g] = left_s[g * span : g * span + LANES, :].astype(bf16)

    peaks[me] = jnp.broadcast_to(jnp.max(jnp.transpose(peak[...]), axis=0, keepdims=True), (8, channels))

    def spread_peak(t, carry):
        peer = lax.rem(me + t, members)
        pltpu.make_async_remote_copy(
            src_ref=peaks.at[me],
            dst_ref=peaks.at[me],
            send_sem=peak_send,
            recv_sem=peak_recv,
            device_id={"gx": peer // ny, "gy": lax.rem(peer, ny)},
            device_id_type=MESH,
        ).start()
        return carry

    lax.fori_loop(1, members, spread_peak, 0)

    lane = lax.broadcasted_iota(jnp.int32, (rows, LANES), 1)

    def triangle_pair(r, p):
        halves = []
        for u in range(2):
            res = lax.dot_general(
                left_b[2 * p + u][:, :cols],
                right_all[r, 2 * p + u],
                (((1,), (0,)), ((), ())),
                preferred_element_type=f32,
            )
            t = res[:rows]
            for s in range(1, per):
                t = jnp.where(lane >= s * rows, res[s * rows : (s + 1) * rows], t)
            halves.append(t)
        return jnp.concatenate(halves, axis=0)

    def x_copy(target, sub, c, source):
        window = pl.ds(bounds[c], bounds[c + 1] - bounds[c])
        return pltpu.make_async_remote_copy(
            src_ref=send_t.at[target, sub, window],
            dst_ref=recv_t.at[source, sub, window],
            send_sem=x_send.at[target, sub, c],
            recv_sem=x_recv.at[source, sub, c],
            device_id={"gy": target},
            device_id_type=MESH,
        )

    def triangle_block(r, c):
        owner, sub = r // ratio, lax.rem(r, ratio)

        @pl.when(owner == y)
        def _():
            for p in range(bounds[c], bounds[c + 1]):
                own_t[sub, p] = triangle_pair(r, p)

        @pl.when(owner != y)
        def _():
            for p in range(bounds[c], bounds[c + 1]):
                send_t[owner, sub, p] = triangle_pair(r, p).astype(bf16)
            x_copy(owner, sub, c, y).start()

    def own_block(c):
        triangle_block(z, c)

    for c in range(chunks):
        own_block(c)

    def gate_step(b, carry):
        for u in range(4):
            i = b * 4 + u
            block = normed[pl.ds(pl.multiple_of(i * cols, 16), LANES), :]
            gating[i] = jax.nn.sigmoid(
                lax.dot_general(
                    gate_ref[...], block, (((1,), (1,)), ((), ())), preferred_element_type=f32
                )
            )
        return carry

    lax.fori_loop(0, rows // 4, gate_step, 0)
    ow_pad[...] = jnp.zeros_like(ow_pad)
    stretch = ow_pad.shape[0] // 2
    square = jnp.concatenate(
        [out_weight_ref[...].astype(f32), jnp.zeros((LANES - half, channels), f32)], axis=0
    )
    turned = jnp.transpose(square)
    for cc in range(2):
        ow_pad[cc * stretch : cc * stretch + half, :] = turned[cc * half : (cc + 1) * half, :]
    for s in range(per):
        parts = [ow_pad[pl.ds(cc * stretch + s, slot, stride=per), :] for cc in range(2)]
        parts.append(jnp.zeros((LANES - 2 * slot, LANES), f32))
        back = jnp.transpose(jnp.concatenate(parts, axis=0))
        mix_w[s * half : (s + 1) * half, :] = back[:half].astype(bf16)
    spread_t[...] = jnp.zeros_like(spread_t)

    def ring_step(d, carry):
        low, high = z - d, z + d
        for c in range(chunks):

            @pl.when(low >= 0)
            def _():
                z_copy(low, c, 0).wait_recv()

                @pl.when(z < nz - 1)
                def _():
                    z_copy(low, c, 0).start()

            @pl.when(high < nz)
            def _():
                z_copy(high, c, 1).wait_recv()

                @pl.when(z > 0)
                def _():
                    z_copy(high, c, 1).start()

            @pl.when(low >= 0)
            def _():
                triangle_block(low, c)

            @pl.when(high < nz)
            def _():
                triangle_block(high, c)

        return carry

    lax.fori_loop(1, nz - 1, ring_step, 0)

    group_lane = lax.broadcasted_iota(jnp.int32, (1, LANES), 1)

    def lane_vector(scalar_of):
        vector = jnp.full((1, LANES), scalar_of(0), f32)
        for s in range(1, per):
            vector = jnp.where(group_lane >= s * rows, scalar_of(s), vector)
        return vector

    def pair_vector(scalar_of, p):
        parts = []
        for u in range(2):
            g = 2 * p + u
            vector = lane_vector(lambda s: scalar_of(g * per + s))
            parts.append(jnp.broadcast_to(vector, (rows, LANES)))
        return jnp.concatenate(parts, axis=0)

    def scale_of(ch):
        ch = jnp.minimum(ch, half - 1)
        return (hist_smem[0, ch] / format_limit) * (hist_smem[1, ch] / format_limit)

    def c_copy(sub, c):
        window = pl.ds(bounds[c], bounds[c + 1] - bounds[c])
        return pltpu.make_async_remote_copy(
            src_ref=full_t.at[col, sub, window],
            dst_ref=full_t.at[col, sub, window],
            send_sem=c_send.at[sub, c],
            recv_sem=c_recv.at[sub, c],
            device_id={"col": 1 - col},
            device_id_type=MESH,
        )

    def send_sub(sub):
        for c in range(chunks):

            def arrive(t, carry):
                x_copy(y, sub, c, lax.rem(y + t, ny)).wait_recv()
                return carry

            lax.fori_loop(1, ny, arrive, 0)

            def finish(p, carry):
                total = own_t[sub, p]
                for t in range(1, ny):
                    total = total + recv_t[lax.rem(y + t, ny), sub, p].astype(f32)
                full_t[col, sub, p] = (total * pair_vector(scale_of, p)).astype(bf16)
                return carry

            lax.fori_loop(bounds[c], bounds[c + 1], finish, 0)
            c_copy(sub, c).start()

    row_at = lax.broadcasted_iota(jnp.int32, (2 * rows, LANES), 0) // rows
    lane_at = lax.broadcasted_iota(jnp.int32, (2 * rows, LANES), 1) // rows
    valid = (((pairs - 1) * 2 + row_at) * per + lane_at) < half

    def segment_mean(pair_sum):
        x = pair_sum[:rows] + pair_sum[rows:]
        total = x
        for s in range(1, per):
            total = total + pltpu.roll(x, s * rows, 1)
        result = total
        for s in range(1, per):
            moved = pltpu.roll(total, LANES - s * rows, 1)
            result = jnp.where(lane < (per - s) * rows, moved, result)
        result = result * (1.0 / channels)
        return jnp.concatenate([result, result], axis=0)

    def norm_sub(sub):
        for c in range(chunks):
            c_copy(sub, c).wait_recv()

        def add_up(p, total):
            return total + full_t[0, sub, p].astype(f32) + full_t[1, sub, p].astype(f32)

        zero = jnp.zeros((2 * rows, LANES), f32)
        mean = segment_mean(lax.fori_loop(0, pairs, add_up, zero))

        def add_squares(p, total):
            for cc in range(2):
                total = total + jnp.square(full_t[cc, sub, p].astype(f32) - mean)
            return total

        squares = lax.fori_loop(0, pairs - 1, add_squares, zero)
        for cc in range(2):
            last = jnp.square(full_t[cc, sub, pairs - 1].astype(f32) - mean)
            squares = squares + jnp.where(valid, last, 0.0)
        factor = lax.rsqrt(segment_mean(squares) + epsilon)

        def normalise(p, carry):
            for cc in range(2):

                def gain_of(ch, cc=cc):
                    return out_gain_smem[cc * half + jnp.minimum(ch, half - 1)]

                def bias_of(ch, cc=cc):
                    return out_bias_smem[cc * half + jnp.minimum(ch, half - 1)]

                t = (full_t[cc, sub, p].astype(f32) - mean) * factor
                t = t * pair_vector(gain_of, p) + pair_vector(bias_of, p)
                for u in range(2):
                    at = (sub * 2 + cc) * slot + 2 * p + u
                    spread_t[pl.ds(at, rows, stride=LANES), :] = t[u * rows : (u + 1) * rows]
            return carry

        lax.fori_loop(0, pairs, normalise, 0)

    order = jnp.where(2 * z >= nz, ratio - 1, 0)
    step_sign = jnp.where(2 * z >= nz, -1, 1)
    for t in range(ratio - 1):
        send_sub(order + step_sign * t)
    for t in range(ratio - 1):
        norm_sub(order + step_sign * t)
    ring_step(nz - 1, 0)
    send_sub(order + step_sign * (ratio - 1))
    norm_sub(order + step_sign * (ratio - 1))

    wide = lax.broadcasted_iota(jnp.int32, (half, LANES), 1)

    def mix_one(i):
        start = pl.multiple_of(i * LANES, LANES)
        tile = spread_t[pl.ds(start, LANES), :].astype(bf16)
        parts = [tile[rr * 2 * slot : (rr + 1) * 2 * slot] for rr in range(ratio)]
        res = jnp.dot(
            mix_w[:, 0 : 2 * slot], jnp.concatenate(parts, axis=1), preferred_element_type=f32
        )
        mixing = None
        for rr in range(ratio):
            total = None
            for s in range(per):
                piece = res[s * half : (s + 1) * half, rr * LANES : (rr + 1) * LANES]
                shift = (rr - s) * rows % LANES
                piece = pltpu.roll(piece, shift, 1) if shift else piece
                total = piece if total is None else total + piece
            mixing = total if mixing is None else jnp.where(wide >= rr * rows, total, mixing)
        out_ref[i] = (gating[i] * mixing)[:, :cols].astype(bf16)

    def mix_step(b, carry):
        for u in range(4):
            mix_one(b * 4 + u)
        return carry

    lax.fori_loop(0, rows // 4, mix_step, 0)

    others = peaks.at[pl.ds(0, members - 1)]
    pltpu.make_async_copy(others, others, peak_recv).wait()
    top = jnp.max(jnp.max(peaks[...], axis=0), axis=0, keepdims=True)
    amax_ref[0:1, :] = top[:, :half]
    amax_ref[1:2, :] = top[:, half:]

    pltpu.make_async_copy(others, others, peak_send).wait()
    for sub in range(ratio):
        for c in range(chunks):
            c_copy(sub, c).wait_send()

    def drain_x(t, carry):
        for sub in range(ratio):
            for c in range(chunks):
                x_copy(lax.rem(y + t, ny), sub, c, y).wait_send()
        return carry

    lax.fori_loop(1, ny, drain_x, 0)

    def drain_z(source, carry):
        for c in range(chunks):

            @pl.when((source <= z) & (z < nz - 1))
            def _():
                z_copy(source, c, 0).wait_send()

            @pl.when((source >= z) & (z > 0))
            def _():
                z_copy(source, c, 1).wait_send()

        return carry

    lax.fori_loop(0, nz, drain_z, 0)


def on_device(
    nz,
    ny,
    pair_rep,
    pair_mask,
    amax_history,
    in_gain,
    in_bias,
    proj_weight,
    gate_weight,
    out_gain,
    out_bias,
    out_weight,
):
    crops, rows, cols, channels = pair_rep.shape
    half = proj_weight.shape[2]
    chunks = 2
    ratio = nz // ny
    per = LANES // rows
    pairs = -(-half // (2 * per))
    groups = 2 * pairs
    slot = LANES // (2 * ratio)
    members = nz * ny
    weights = jnp.transpose(proj_weight, (1, 2, 0)).reshape(4 * half, channels)
    scratch_rows = -(-((groups - 1) * per * rows + LANES) // 8) * 8
    dma = pltpu.SemaphoreType.DMA
    vmem = pl.BlockSpec(memory_space=pltpu.VMEM)
    smem = pl.BlockSpec(memory_space=pltpu.SMEM)
    tile = (2 * rows, LANES)
    update, new_amax = pl.pallas_call(
        functools.partial(kernel, (nz, ny, rows, cols, half, chunks)),
        out_shape=(
            jax.ShapeDtypeStruct((rows, half, cols), bf16),
            jax.ShapeDtypeStruct((2, half), f32),
        ),
        in_specs=[vmem, vmem, vmem, smem, vmem, vmem, vmem, vmem, smem, smem, vmem],
        out_specs=(vmem, vmem),
        scratch_shapes=[
            pltpu.VMEM((rows * cols + LANES, channels), bf16),
            pltpu.VMEM((rows, LANES), f32),
            pltpu.VMEM((channels, LANES), f32),
            pltpu.VMEM((channels, LANES), f32),
            pltpu.VMEM((scratch_rows, LANES), f32),
            pltpu.VMEM((scratch_rows, LANES), f32),
            pltpu.VMEM((groups, LANES, LANES), bf16),
            pltpu.VMEM((nz, groups, cols, LANES), bf16),
            pltpu.VMEM((ratio, pairs) + tile, f32),
            pltpu.VMEM((ny, ratio, pairs) + tile, bf16),
            pltpu.VMEM((ny, ratio, pairs) + tile, bf16),
            pltpu.VMEM((2, ratio, pairs) + tile, bf16),
            pltpu.VMEM((rows * LANES, LANES), f32),
            pltpu.VMEM((per * half, LANES), bf16),
            pltpu.VMEM((2 * slot * per, LANES), f32),
            pltpu.VMEM((rows, half, LANES), f32),
            pltpu.VMEM((members, 8, channels), f32),
            dma,
            dma,
            dma((2, nz, chunks)),
            dma((nz, chunks)),
            dma((ny, ratio, chunks)),
            dma((ny, ratio, chunks)),
            dma((ratio, chunks)),
            dma((ratio, chunks)),
        ],
        compiler_params=pltpu.CompilerParams(
            collective_id=0, has_side_effects=True, vmem_limit_bytes=56 * 1024 * 1024
        ),
    )(
        pair_rep[0],
        pair_mask[0],
        amax_history,
        amax_history,
        in_gain.reshape(1, channels),
        in_bias.reshape(1, channels),
        weights,
        gate_weight.T,
        out_gain,
        out_bias,
        out_weight.T,
    )
    return jnp.transpose(update, (0, 2, 1))[None], new_amax


def solution(mesh):
    placed = (
        P("ga", "gx", "gy", None),
        P("ga", "gx", "gy"),
        P(None, "col"),
        P(),
        P(),
        P(None, None, "col"),
        P(None, "col"),
        P(),
        P(),
        P(None, "col"),
    )
    return jax.shard_map(
        functools.partial(on_device, mesh.shape["gx"], mesh.shape["gy"]),
        mesh=mesh,
        in_specs=placed,
        out_specs=(P("ga", "gx", "gy", "col"), P("ga", "col")),
        check_vma=False,
    )
```

```python
import functools

import jax
import jax.numpy as jnp
from jax import lax
from jax.experimental import pallas as pl
from jax.experimental.pallas import tpu as pltpu
from jax.sharding import PartitionSpec as P

epsilon = 1e-05
format_limit = 448.0
LANES = 128
f32, bf16 = jnp.float32, jnp.bfloat16
MESH = pl.DeviceIdType.MESH


def kernel(
    dims,
    rep_ref,
    mask_ref,
    hist_ref,
    hist_smem,
    in_gain_ref,
    in_bias_ref,
    proj_ref,
    gate_ref,
    out_gain_smem,
    out_bias_smem,
    out_weight_ref,
    out_ref,
    amax_ref,
    normed,
    maskf,
    inverse,
    peak,
    left_s,
    right_s,
    left_b,
    left_t,
    left_e,
    edge_t,
    edge_in,
    right_all,
    own_t,
    send_t,
    recv_t,
    full_t,
    spread_t,
    mix_w,
    ow_pad,
    gating,
    mixed,
    out_v,
    out_sem,
    peaks,
    peak_send,
    peak_recv,
    z_send,
    z_recv,
    x_send,
    x_recv,
    c_send,
    c_recv,
    left_send,
    left_recv,
    edge_send,
    edge_recv,
):
    nz, ny, rows, cols, half, chunks = dims
    ratio = nz // ny
    channels = 2 * half
    per = LANES // rows
    pairs = -(-half // (2 * per))
    groups = 2 * pairs
    span = per * rows
    slot = LANES // (2 * ratio)
    z, y, col = lax.axis_index("gx"), lax.axis_index("gy"), lax.axis_index("col")
    members = nz * ny
    me = z * ny + y

    barrier = pltpu.get_barrier_semaphore()

    def greet(t, carry):
        peer = lax.rem(me + t, members)
        pl.semaphore_signal(
            barrier, inc=1, device_id={"gx": peer // ny, "gy": lax.rem(peer, ny)}, device_id_type=MESH
        )
        return carry

    lax.fori_loop(1, members, greet, 0)
    pl.semaphore_signal(barrier, inc=1, device_id={"col": 1 - col}, device_id_type=MESH)

    normed[pl.ds(rows * cols, LANES), :] = jnp.zeros((LANES, channels), bf16)
    step_rows = 4

    def norm_step(b, carry):
        values = rep_ref[pl.ds(b * step_rows, step_rows)].reshape(step_rows * cols, channels).astype(f32)
        average = jnp.mean(values, axis=-1, keepdims=True)
        centred = values - average
        var = jnp.mean(jnp.square(centred), axis=-1, keepdims=True)
        result = centred * lax.rsqrt(var + epsilon) * in_gain_ref[...] + in_bias_ref[...]
        start = pl.multiple_of(b * step_rows * cols, 16)
        normed[pl.ds(start, step_rows * cols), :] = result.astype(bf16)
        return carry

    lax.fori_loop(0, rows // step_rows, norm_step, 0)
    maskf[...] = jnp.zeros_like(maskf)
    maskf[:, 0:cols] = mask_ref[...].astype(f32)
    scaled = format_limit / hist_ref[...]
    flipped = jnp.concatenate([scaled[0:1], scaled[1:2]], axis=1)
    flipped = jnp.broadcast_to(flipped, (channels, channels))
    inverse[...] = jnp.transpose(flipped)
    peak[...] = jnp.zeros_like(peak)
    tail = left_s.shape[0] - half * rows
    left_s[pl.ds(half * rows, tail), :] = jnp.zeros((tail, LANES), f32)
    right_s[pl.ds(half * rows, tail), :] = jnp.zeros((tail, LANES), f32)

    def project(side, target):
        base = side * half

        def one(i):
            block = normed[pl.ds(pl.multiple_of(i * cols, 16), LANES), :]
            p = lax.dot_general(
                proj_ref[2 * base : 2 * base + channels, :],
                block,
                (((1,), (1,)), ((), ())),
                preferred_element_type=f32,
            )
            value = jax.nn.sigmoid(p[half:]) * p[:half] * maskf[pl.ds(i, 1), :]
            target[pl.ds(i, half, stride=rows), :] = jnp.clip(
                value * inverse[base : base + half, :], -format_limit, format_limit
            )
            return jnp.abs(value)

        def step(b, top):
            for u in range(4):
                top = jnp.maximum(top, one(b * 4 + u))
            return top

        top = lax.fori_loop(0, rows // 4, step, jnp.zeros((half, LANES), f32))
        peak[base : base + half, :] = top

    project(1, right_s)
    bounds = [pairs * c // chunks for c in range(chunks + 1)]

    def z_copy(source, c, direction):
        window = pl.ds(2 * bounds[c], 2 * (bounds[c + 1] - bounds[c]))
        toward = z + 1 if direction == 0 else z - 1
        return pltpu.make_async_remote_copy(
            src_ref=right_all.at[source, window],
            dst_ref=right_all.at[source, window],
            send_sem=z_send.at[direction, source, c],
            recv_sem=z_recv.at[source, c],
            device_id={"gx": toward},
            device_id_type=MESH,
        )

    pl.semaphore_wait(barrier, members)
    for c in range(chunks):
        for g in range(2 * bounds[c], 2 * bounds[c + 1]):
            tile = jnp.transpose(right_s[g * span : g * span + LANES, :])
            right_all[z, g] = tile[:cols].astype(bf16)

        @pl.when(z < nz - 1)
        def _():
            z_copy(z, c, 0).start()

        @pl.when(z > 0)
        def _():
            z_copy(z, c, 1).start()

    project(0, left_s)
    for g in range(groups):
        left_b[g] = left_s[g * span : g * span + LANES, :].astype(bf16)

    is_end = (z == 0) | (z == nz - 1)
    is_next = (z == 1) | (z == nz - 2)
    upper = 2 * z >= nz
    inward = jnp.where(upper, z - 1, z + 1)
    outward = jnp.where(upper, z + 1, z - 1)
    far = jnp.where(upper, 0, nz - 1)

    def left_copy(c):
        window = pl.ds(2 * bounds[c], 2 * (bounds[c + 1] - bounds[c]))
        return pltpu.make_async_remote_copy(
            src_ref=left_t.at[window],
            dst_ref=left_e.at[window],
            send_sem=left_send.at[c],
            recv_sem=left_recv.at[c],
            device_id={"gx": inward},
            device_id_type=MESH,
        )

    def edge_copy(c):
        window = pl.ds(bounds[c], bounds[c + 1] - bounds[c])
        return pltpu.make_async_remote_copy(
            src_ref=edge_t.at[window],
            dst_ref=edge_in.at[window],
            send_sem=edge_send.at[c],
            recv_sem=edge_recv.at[c],
            device_id={"gx": outward},
            device_id_type=MESH,
        )

    @pl.when(is_end)
    def _():
        for c in range(chunks):
            for g in range(2 * bounds[c], 2 * bounds[c + 1]):
                tile = jnp.transpose(left_s[g * span : g * span + LANES, :])
                left_t[g] = tile[:cols].astype(bf16)
            left_copy(c).start()

    peaks[me] = jnp.broadcast_to(jnp.max(jnp.transpose(peak[...]), axis=0, keepdims=True), (8, channels))

    def spread_peak(t, carry):
        peer = lax.rem(me + t, members)
        pltpu.make_async_remote_copy(
            src_ref=peaks.at[me],
            dst_ref=peaks.at[me],
            send_sem=peak_send,
            recv_sem=peak_recv,
            device_id={"gx": peer // ny, "gy": lax.rem(peer, ny)},
            device_id_type=MESH,
        ).start()
        return carry

    lax.fori_loop(1, members, spread_peak, 0)

    lane = lax.broadcasted_iota(jnp.int32, (rows, LANES), 1)

    def triangle_pair(r, p, edge=False):
        halves = []
        for u in range(2):
            if edge:
                tile = jnp.transpose(left_e[2 * p + u].astype(f32)).astype(bf16)
            else:
                tile = left_b[2 * p + u][:, :cols]
            res = lax.dot_general(
                tile,
                right_all[r, 2 * p + u],
                (((1,), (0,)), ((), ())),
                preferred_element_type=f32,
            )
            t = res[:rows]
            for s in range(1, per):
                t = jnp.where(lane >= s * rows, res[s * rows : (s + 1) * rows], t)
            halves.append(t)
        return jnp.concatenate(halves, axis=0)

    def x_copy(target, sub, c, source):
        window = pl.ds(bounds[c], bounds[c + 1] - bounds[c])
        return pltpu.make_async_remote_copy(
            src_ref=send_t.at[target, sub, window],
            dst_ref=recv_t.at[source, sub, window],
            send_sem=x_send.at[target, sub, c],
            recv_sem=x_recv.at[source, sub, c],
            device_id={"gy": target},
            device_id_type=MESH,
        )

    def triangle_block(r, c):
        owner, sub = r // ratio, lax.rem(r, ratio)

        @pl.when(owner == y)
        def _():
            for p in range(bounds[c], bounds[c + 1]):
                own_t[sub, p] = triangle_pair(r, p)

        @pl.when(owner != y)
        def _():
            for p in range(bounds[c], bounds[c + 1]):
                send_t[owner, sub, p] = triangle_pair(r, p).astype(bf16)
            x_copy(owner, sub, c, y).start()

    def own_block(c):
        triangle_block(z, c)

    for c in range(chunks):
        own_block(c)

    def gate_step(b, carry):
        for u in range(4):
            i = b * 4 + u
            block = normed[pl.ds(pl.multiple_of(i * cols, 16), LANES), :]
            gating[i] = jax.nn.sigmoid(
                lax.dot_general(
                    gate_ref[...], block, (((1,), (1,)), ((), ())), preferred_element_type=f32
                )
            )
        return carry

    lax.fori_loop(0, rows // 4, gate_step, 0)
    ow_pad[...] = jnp.zeros_like(ow_pad)
    stretch = ow_pad.shape[0] // 2
    square = jnp.concatenate(
        [out_weight_ref[...].astype(f32), jnp.zeros((LANES - half, channels), f32)], axis=0
    )
    turned = jnp.transpose(square)
    for cc in range(2):
        ow_pad[cc * stretch : cc * stretch + half, :] = turned[cc * half : (cc + 1) * half, :]
    for s in range(per):
        parts = [ow_pad[pl.ds(cc * stretch + s, slot, stride=per), :] for cc in range(2)]
        parts.append(jnp.zeros((LANES - 2 * slot, LANES), f32))
        back = jnp.transpose(jnp.concatenate(parts, axis=0))
        mix_w[s * half : (s + 1) * half, :] = back[:half].astype(bf16)
    spread_t[...] = jnp.zeros_like(spread_t)

    def ring_step(d, carry):
        low, high = z - d, z + d
        for c in range(chunks):

            @pl.when(low >= 0)
            def _():
                z_copy(low, c, 0).wait_recv()

                @pl.when((z < nz - 1) & ((z < nz - 2) | (low > 0)))
                def _():
                    z_copy(low, c, 0).start()

            @pl.when(high < nz)
            def _():
                z_copy(high, c, 1).wait_recv()

                @pl.when((z > 0) & ((z > 1) | (high < nz - 1)))
                def _():
                    z_copy(high, c, 1).start()

            @pl.when(low >= 0)
            def _():
                triangle_block(low, c)

            @pl.when(high < nz)
            def _():
                triangle_block(high, c)

            @pl.when((d == nz - 2) & is_next)
            def _():
                left_copy(c).wait_recv()
                for p in range(bounds[c], bounds[c + 1]):
                    edge_t[p] = triangle_pair(far, p, True).astype(bf16)
                edge_copy(c).start()

        return carry

    def edge_step():
        owner, sub = far // ratio, lax.rem(far, ratio)
        for c in range(chunks):
            window = pl.ds(bounds[c], bounds[c + 1] - bounds[c])
            edge_copy(c).wait_recv()

            @pl.when(owner == y)
            def _():
                own_t[sub, window] = edge_in[window].astype(f32)

            @pl.when(owner != y)
            def _():
                pltpu.make_async_remote_copy(
                    src_ref=edge_in.at[window],
                    dst_ref=recv_t.at[y, sub, window],
                    send_sem=x_send.at[owner, sub, c],
                    recv_sem=x_recv.at[y, sub, c],
                    device_id={"gy": owner},
                    device_id_type=MESH,
                ).start()

    lax.fori_loop(1, nz - 1, ring_step, 0)

    group_lane = lax.broadcasted_iota(jnp.int32, (1, LANES), 1)

    def lane_vector(scalar_of):
        vector = jnp.full((1, LANES), scalar_of(0), f32)
        for s in range(1, per):
            vector = jnp.where(group_lane >= s * rows, scalar_of(s), vector)
        return vector

    def pair_vector(scalar_of, p):
        parts = []
        for u in range(2):
            g = 2 * p + u
            vector = lane_vector(lambda s: scalar_of(g * per + s))
            parts.append(jnp.broadcast_to(vector, (rows, LANES)))
        return jnp.concatenate(parts, axis=0)

    def scale_of(ch):
        ch = jnp.minimum(ch, half - 1)
        return (hist_smem[0, ch] / format_limit) * (hist_smem[1, ch] / format_limit)

    def c_copy(sub, c):
        window = pl.ds(bounds[c], bounds[c + 1] - bounds[c])
        return pltpu.make_async_remote_copy(
            src_ref=full_t.at[col, sub, window],
            dst_ref=full_t.at[col, sub, window],
            send_sem=c_send.at[sub, c],
            recv_sem=c_recv.at[sub, c],
            device_id={"col": 1 - col},
            device_id_type=MESH,
        )

    def send_sub(sub):
        for c in range(chunks):

            def arrive(t, carry):
                x_copy(y, sub, c, lax.rem(y + t, ny)).wait_recv()
                return carry

            lax.fori_loop(1, ny, arrive, 0)

            def finish(p, carry):
                total = own_t[sub, p]
                for t in range(1, ny):
                    total = total + recv_t[lax.rem(y + t, ny), sub, p].astype(f32)
                full_t[col, sub, p] = (total * pair_vector(scale_of, p)).astype(bf16)
                return carry

            lax.fori_loop(bounds[c], bounds[c + 1], finish, 0)
            c_copy(sub, c).start()

    row_at = lax.broadcasted_iota(jnp.int32, (2 * rows, LANES), 0) // rows
    lane_at = lax.broadcasted_iota(jnp.int32, (2 * rows, LANES), 1) // rows
    valid = (((pairs - 1) * 2 + row_at) * per + lane_at) < half

    def segment_mean(pair_sum):
        x = pair_sum[:rows] + pair_sum[rows:]
        total = x
        for s in range(1, per):
            total = total + pltpu.roll(x, s * rows, 1)
        result = total
        for s in range(1, per):
            moved = pltpu.roll(total, LANES - s * rows, 1)
            result = jnp.where(lane < (per - s) * rows, moved, result)
        result = result * (1.0 / channels)
        return jnp.concatenate([result, result], axis=0)

    def norm_sub(sub):
        for c in range(chunks):
            c_copy(sub, c).wait_recv()

        def add_up(p, total):
            return total + full_t[0, sub, p].astype(f32) + full_t[1, sub, p].astype(f32)

        zero = jnp.zeros((2 * rows, LANES), f32)
        mean = segment_mean(lax.fori_loop(0, pairs, add_up, zero))

        def add_squares(p, total):
            for cc in range(2):
                total = total + jnp.square(full_t[cc, sub, p].astype(f32) - mean)
            return total

        squares = lax.fori_loop(0, pairs - 1, add_squares, zero)
        for cc in range(2):
            last = jnp.square(full_t[cc, sub, pairs - 1].astype(f32) - mean)
            squares = squares + jnp.where(valid, last, 0.0)
        factor = lax.rsqrt(segment_mean(squares) + epsilon)

        def normalise(p, carry):
            for cc in range(2):

                def gain_of(ch, cc=cc):
                    return out_gain_smem[cc * half + jnp.minimum(ch, half - 1)]

                def bias_of(ch, cc=cc):
                    return out_bias_smem[cc * half + jnp.minimum(ch, half - 1)]

                t = (full_t[cc, sub, p].astype(f32) - mean) * factor
                t = t * pair_vector(gain_of, p) + pair_vector(bias_of, p)
                for u in range(2):
                    at = (sub * 2 + cc) * slot + 2 * p + u
                    spread_t[pl.ds(at, rows, stride=LANES), :] = t[u * rows : (u + 1) * rows]
            return carry

        lax.fori_loop(0, pairs, normalise, 0)

    wide = lax.broadcasted_iota(jnp.int32, (half, LANES), 1)

    def mix_sub(sub, last):
        def two_rows(i):
            parts = []
            for u in range(2):
                start = pl.multiple_of((i + u) * LANES + sub * (2 * slot), 2 * slot)
                parts.append(spread_t[pl.ds(start, 2 * slot), :].astype(bf16))
            res = jnp.dot(
                mix_w[:, 0 : 2 * slot], jnp.concatenate(parts, axis=1), preferred_element_type=f32
            )
            for u in range(2):
                total = res[:half, u * LANES : (u + 1) * LANES]
                for s in range(1, per):
                    piece = res[s * half : (s + 1) * half, u * LANES : (u + 1) * LANES]
                    total = total + pltpu.roll(piece, LANES - s * rows, 1)
                mixed[sub, i + u] = total

        def out_row(i):
            mixing = mixed[0, i]
            for rr in range(1, ratio):
                moved = pltpu.roll(mixed[rr, i], rr * rows, 1)
                mixing = jnp.where(wide >= rr * rows, moved, mixing)
            out_v[i] = (gating[i] * mixing)[:, :cols].astype(bf16)

        def mix_step(b, carry):
            for u in range(2):
                two_rows(b * 4 + 2 * u)
            if last:
                for u in range(4):
                    out_row(b * 4 + u)
                out_copy(b).start()
            return carry

        lax.fori_loop(0, rows // 4, mix_step, 0)

    def out_copy(b):
        window = pl.ds(b * 4, 4)
        return pltpu.make_async_copy(out_v.at[window], out_ref.at[window], out_sem.at[b])

    order = jnp.where(2 * z >= nz, ratio - 1, 0)
    step_sign = jnp.where(2 * z >= nz, -1, 1)
    for t in range(ratio - 1):
        send_sub(order + step_sign * t)
    for t in range(ratio - 1):
        norm_sub(order + step_sign * t)
        mix_sub(order + step_sign * t, False)
    pl.when(is_end)(edge_step)
    send_sub(order + step_sign * (ratio - 1))
    norm_sub(order + step_sign * (ratio - 1))
    mix_sub(order + step_sign * (ratio - 1), True)

    others = peaks.at[pl.ds(0, members - 1)]
    pltpu.make_async_copy(others, others, peak_recv).wait()
    top = jnp.max(jnp.max(peaks[...], axis=0), axis=0, keepdims=True)
    amax_ref[0:1, :] = top[:, :half]
    amax_ref[1:2, :] = top[:, half:]

    def drain_out(b, carry):
        out_copy(b).wait()
        return carry

    lax.fori_loop(0, rows // 4, drain_out, 0)

    pltpu.make_async_copy(others, others, peak_send).wait()
    for sub in range(ratio):
        for c in range(chunks):
            c_copy(sub, c).wait_send()

    def drain_x(t, carry):
        for sub in range(ratio):
            for c in range(chunks):
                x_copy(lax.rem(y + t, ny), sub, c, y).wait_send()
        return carry

    lax.fori_loop(1, ny, drain_x, 0)

    def drain_z(source, carry):
        for c in range(chunks):

            @pl.when((source <= z) & (z < nz - 1) & ((z < nz - 2) | (source > 0)))
            def _():
                z_copy(source, c, 0).wait_send()

            @pl.when((source >= z) & (z > 0) & ((z > 1) | (source < nz - 1)))
            def _():
                z_copy(source, c, 1).wait_send()

        return carry

    lax.fori_loop(0, nz, drain_z, 0)

    @pl.when(is_end)
    def _():
        for c in range(chunks):
            left_copy(c).wait_send()

    @pl.when(is_next)
    def _():
        for c in range(chunks):
            edge_copy(c).wait_send()


def on_device(
    nz,
    ny,
    pair_rep,
    pair_mask,
    amax_history,
    in_gain,
    in_bias,
    proj_weight,
    gate_weight,
    out_gain,
    out_bias,
    out_weight,
):
    crops, rows, cols, channels = pair_rep.shape
    half = proj_weight.shape[2]
    chunks = 4
    ratio = nz // ny
    per = LANES // rows
    pairs = -(-half // (2 * per))
    groups = 2 * pairs
    slot = LANES // (2 * ratio)
    members = nz * ny
    weights = jnp.transpose(proj_weight, (1, 2, 0)).reshape(4 * half, channels)
    scratch_rows = -(-((groups - 1) * per * rows + LANES) // 8) * 8
    dma = pltpu.SemaphoreType.DMA
    vmem = pl.BlockSpec(memory_space=pltpu.VMEM)
    smem = pl.BlockSpec(memory_space=pltpu.SMEM)
    tile = (2 * rows, LANES)
    update, new_amax = pl.pallas_call(
        functools.partial(kernel, (nz, ny, rows, cols, half, chunks)),
        out_shape=(
            jax.ShapeDtypeStruct((rows, half, cols), bf16),
            jax.ShapeDtypeStruct((2, half), f32),
        ),
        in_specs=[vmem, vmem, vmem, smem, vmem, vmem, vmem, vmem, smem, smem, vmem],
        out_specs=(pl.BlockSpec(memory_space=pl.ANY), vmem),
        scratch_shapes=[
            pltpu.VMEM((rows * cols + LANES, channels), bf16),
            pltpu.VMEM((rows, LANES), f32),
            pltpu.VMEM((channels, LANES), f32),
            pltpu.VMEM((channels, LANES), f32),
            pltpu.VMEM((scratch_rows, LANES), f32),
            pltpu.VMEM((scratch_rows, LANES), f32),
            pltpu.VMEM((groups, LANES, LANES), bf16),
            pltpu.VMEM((groups, cols, LANES), bf16),
            pltpu.VMEM((groups, cols, LANES), bf16),
            pltpu.VMEM((pairs,) + tile, bf16),
            pltpu.VMEM((pairs,) + tile, bf16),
            pltpu.VMEM((nz, groups, cols, LANES), bf16),
            pltpu.VMEM((ratio, pairs) + tile, f32),
            pltpu.VMEM((ny, ratio, pairs) + tile, bf16),
            pltpu.VMEM((ny, ratio, pairs) + tile, bf16),
            pltpu.VMEM((2, ratio, pairs) + tile, bf16),
            pltpu.VMEM((rows * LANES, LANES), f32),
            pltpu.VMEM((per * half, LANES), bf16),
            pltpu.VMEM((2 * slot * per, LANES), f32),
            pltpu.VMEM((rows, half, LANES), f32),
            pltpu.VMEM((ratio, rows, half, LANES), f32),
            pltpu.VMEM((rows, half, cols), bf16),
            dma((rows // 4,)),
            pltpu.VMEM((members, 8, channels), f32),
            dma,
            dma,
            dma((2, nz, chunks)),
            dma((nz, chunks)),
            dma((ny, ratio, chunks)),
            dma((ny, ratio, chunks)),
            dma((ratio, chunks)),
            dma((ratio, chunks)),
            dma((chunks,)),
            dma((chunks,)),
            dma((chunks,)),
            dma((chunks,)),
        ],
        compiler_params=pltpu.CompilerParams(
            collective_id=0, has_side_effects=True, vmem_limit_bytes=56 * 1024 * 1024
        ),
    )(
        pair_rep[0],
        pair_mask[0],
        amax_history,
        amax_history,
        in_gain.reshape(1, channels),
        in_bias.reshape(1, channels),
        weights,
        gate_weight.T,
        out_gain,
        out_bias,
        out_weight.T,
    )
    return jnp.transpose(update, (0, 2, 1))[None], new_amax


def solution(mesh):
    placed = (
        P("ga", "gx", "gy", None),
        P("ga", "gx", "gy"),
        P(None, "col"),
        P(),
        P(),
        P(None, None, "col"),
        P(None, "col"),
        P(),
        P(),
        P(None, "col"),
    )
    return jax.shard_map(
        functools.partial(on_device, mesh.shape["gx"], mesh.shape["gy"]),
        mesh=mesh,
        in_specs=placed,
        out_specs=(P("ga", "gx", "gy", "col"), P("ga", "col")),
        check_vma=False,
    )
```
